32 devices in a mesh: ga: 8 (over z, x), band: 4 (over y, core).
Axes of the slice: x: 2, y: 2, z: 4, core: 2. Of those that a mesh axis runs over, the one named last changes fastest.
Arguments:
- coeffs: bfloat16 [2, 512, 40960], P(None, ('ga', 'band')), may hold values from -6 to 6
- projectors: bfloat16 [1280, 2, 40960], P(None, None, 'ga'), may hold values from -0.01953125 to 0.01953125
- block_coupling: float32 [1280, 18], replicated, may hold values from -12 to 12
- atom_counts: int32 [160], replicated, may hold values from 4 to 18, as said below
- wave_counts: int32 [8], P('ga'), may hold values from 3840 to 5120
Outputs:
- applied: bfloat16 [2, 512, 40960], P(None, ('ga', 'band'))
- band_energy: float32 [512], P(('ga', 'band'))
- total_energy: float32 [], replicated
The draws below stay inside these ranges and needn't reach their ends.
Inputs may be any that keep to these rules, and one draw needn't show every extreme that they name: `atom_counts`: each atom has 4, 8 or 18 projectors, the counts sum to 1280 and the largest is 18.
All inputs are finite; a program needn't handle non-finite values.
Results may differ from the reference program's by a relative error of at most 0.013.
Values may be sent and summed in bfloat16 or wider, within the bound.
No kernel may reach another device: no remote copies, remote signals or barrier semaphores. Data moves between devices by JAX's collectives and lax.ppermute only.
A program may use at most 128 MiB of HBM per device.

```python
import math
import jax
import jax.numpy as jnp
from jax import lax

NG = 40960
ATOMS = 160
MOST = 18
G_DEV = 5120
NB = 512
NP = 1280
N_GA = 8


def draw_atom_counts(key, part):
    group_pattern = jnp.array([18, 18, 4, 4, 4, 4, 4], jnp.int32)
    heavy_groups = ATOMS // 8
    atom_ids = lax.iota(jnp.int32, ATOMS)
    species = jnp.where(atom_ids < 7 * heavy_groups, group_pattern[atom_ids % 7], 8).astype(jnp.int32)
    return jax.random.permutation(jax.random.fold_in(key, 31), species).astype(jnp.int32)


def with_ends(entries, key, smallest, largest):
    spot = [jax.random.randint(jax.random.fold_in(key, axis), (), 0, length) for axis, length in enumerate(entries.shape)]
    widest = entries.shape.index(max(entries.shape))
    next_to = spot[:widest] + [(spot[widest] + 1) % entries.shape[widest]] + spot[widest + 1:]
    return entries.at[tuple(spot)].set(smallest).at[tuple(next_to)].set(largest)


def level_of(stream_key, extent, cuts, smallest, largest):
    loudness = 1.0
    for axis_at, shards_of in cuts:
        steps = jax.random.uniform(jax.random.fold_in(jax.random.fold_in(stream_key, 6), axis_at), (shards_of,), jnp.float32, smallest / len(cuts), largest / len(cuts))
        loudness = loudness * jnp.repeat(jnp.exp(steps), extent[axis_at] // shards_of).reshape((-1,) + (1,) * (len(extent) - 1 - axis_at))
    return loudness


def noise(own_key, extent, spread, most, pieces=(), kind=jnp.bfloat16):
    gain = level_of(own_key, extent, pieces, -0.22, 0.18) if pieces else 1.0
    values = jax.random.normal(own_key, extent, jnp.float32) * spread * gain
    return jnp.minimum(jnp.maximum(values, -most), most).astype(kind)


def setup_inputs(seed: int = 0) -> dict:
    streams_of = jax.random.split(jax.random.key(seed), 6)
    return {
        "coeffs": noise(streams_of[0], (2, NB, NG), 1.0, 6.0, ((1, 32),)),
        "projectors": noise(streams_of[1], (NP, 2, NG), (2 * NG) ** -0.5, 0.01953125, ((2, 8),)),
        "block_coupling": noise(streams_of[2], (NP, MOST), 2.0, 12.0, (), jnp.float32),
        "atom_counts": draw_atom_counts(jax.random.fold_in(streams_of[5], 71), 0),
        "wave_counts": with_ends(jax.random.randint(streams_of[4], (N_GA,), G_DEV * 3 // 4, G_DEV + 1), jax.random.fold_in(streams_of[4], 1), G_DEV * 3 // 4, G_DEV).astype(jnp.int32),
    }


def block_tables(atom_counts, row_ids):
    atom_ends = jnp.cumsum(atom_counts).astype(jnp.int32)
    atom_starts = (atom_ends - atom_counts).astype(jnp.int32)
    inside = (atom_starts[None, :] <= row_ids[:, None]) & (atom_ends[None, :] > row_ids[:, None])
    block_first = lax.optimization_barrier(jnp.sum(jnp.where(inside, atom_starts[None, :], 0), axis=1)).astype(jnp.int32)
    block_length = lax.optimization_barrier(jnp.sum(jnp.where(inside, atom_counts[None, :], 0), axis=1)).astype(jnp.int32)
    return (block_first, block_length)

def couple_rows(values, block_first, block_length, coupling_rows, row_base):
    last_row = values.shape[0] - 1
    summed = jnp.zeros((coupling_rows.shape[0], values.shape[1]), jnp.float32)
    for offset in range(coupling_rows.shape[1]):
        source = jnp.clip(block_first + offset - row_base, 0, last_row).astype(jnp.int32)
        column = coupling_rows[:, offset]
        weight = jnp.where(offset < block_length, column, jnp.zeros_like(column))
        summed = summed + weight[:, None] * jnp.take(values, source, axis=0)
    return summed

def reference(coeffs, projectors, block_coupling, atom_counts, wave_counts):
    slot_ids = lax.iota(jnp.int32, NG)
    in_sphere = (slot_ids % G_DEV < wave_counts[slot_ids // G_DEV]).astype(jnp.float32)
    masked = coeffs * in_sphere.astype(coeffs.dtype)
    real_part = masked[0]
    imag_part = masked[1]
    stacked = jnp.concatenate([jnp.concatenate([real_part, imag_part], 1), jnp.concatenate([imag_part, -real_part], 1)], 0)
    flat_beta = projectors.reshape(NP, 2 * NG)
    projections = lax.dot_general(flat_beta, stacked, (((1,), (1,)), ((), ())), preferred_element_type=jnp.float32)
    block_first, block_length = block_tables(atom_counts, lax.iota(jnp.int32, NP))
    coupled = couple_rows(projections, block_first, block_length, block_coupling, 0)
    energy_terms = lax.optimization_barrier(jnp.sum(projections * coupled, axis=0))
    band_energy = (energy_terms[:NB] + energy_terms[NB:]) / NP
    total_energy = jnp.sum(band_energy) / math.sqrt(NB)
    products = lax.dot_general(coupled.astype(jnp.bfloat16), flat_beta, (((0,), (0,)), ((), ())), preferred_element_type=jnp.float32)
    real_out = products[:NB, :NG] - products[NB:, NG:]
    imag_out = products[:NB, NG:] + products[NB:, :NG]
    applied = (jnp.stack([real_out, imag_out]) * in_sphere).astype(jnp.bfloat16)
    return (applied, band_energy, total_energy)
```

```python
import math

import jax
import jax.numpy as jnp
from jax import lax
from jax.experimental import pallas as pl
from jax.experimental.pallas import tpu as pltpu
from jax.sharding import PartitionSpec as P


def block_tables(atom_counts, row_ids):
    atom_ends = jnp.cumsum(atom_counts)
    atom_starts = atom_ends - atom_counts
    inside = (atom_starts[None, :] <= row_ids[:, None]) & (atom_ends[None, :] > row_ids[:, None])
    block_first = jnp.sum(jnp.where(inside, atom_starts[None, :], 0), axis=1)
    block_length = jnp.sum(jnp.where(inside, atom_counts[None, :], 0), axis=1)
    return (block_first, block_length)


def shift_weights(block_first, block_length, coupling):
    rows, most = coupling.shape
    columns = coupling.T
    shifts = lax.iota(jnp.int32, 2 * most - 1) - (most - 1)
    place = shifts[:, None] + (lax.iota(jnp.int32, rows) - block_first)[None, :]
    weights = jnp.zeros(place.shape, jnp.float32)
    for k in range(most):
        hit = (place == k) & (k < block_length)[None, :]
        weights = jnp.where(hit, columns[k][None, :], weights)
    return weights


def project(moved, beta, wave_counts, tile):
    sources, _, bands, slots = moved.shape
    rows = sources * 2 * bands
    count = beta.shape[1]

    def kernel(counts_ref, x_ref, beta_ref, out_ref, masked_ref):
        @pl.when(pl.program_id(0) == 0)
        def _():
            inside = lax.broadcasted_iota(jnp.int32, (2 * bands, slots), 1) < counts_ref[0]
            for s in range(sources):
                part = x_ref[s].reshape(2 * bands, slots)
                masked_ref[s * 2 * bands : (s + 1) * 2 * bands, :] = jnp.where(inside, part, jnp.zeros_like(part))

        nt = (((1,), (1,)), ((), ()))
        masked = masked_ref[...]
        first = lax.dot_general(masked, beta_ref[0], nt, preferred_element_type=jnp.float32)
        second = lax.dot_general(masked, beta_ref[1], nt, preferred_element_type=jnp.float32)
        for s in range(sources):
            re = slice(s * 2 * bands, s * 2 * bands + bands)
            im = slice(s * 2 * bands + bands, (s + 1) * 2 * bands)
            out_ref[s, :bands, :] = first[re] + second[im]
            out_ref[s, bands:, :] = first[im] - second[re]

    return pl.pallas_call(
        kernel,
        grid_spec=pltpu.PrefetchScalarGridSpec(
            num_scalar_prefetch=1,
            grid=(count // tile,),
            in_specs=[
                pl.BlockSpec((sources, 2, bands, slots), lambda i, c: (0, 0, 0, 0)),
                pl.BlockSpec((2, tile, slots), lambda i, c: (0, i, 0)),
            ],
            out_specs=pl.BlockSpec((sources, 2 * bands, tile), lambda i, c: (0, 0, i)),
            scratch_shapes=[pltpu.VMEM((rows, slots), jnp.bfloat16)],
        ),
        out_shape=jax.ShapeDtypeStruct((sources, 2 * bands, count), jnp.float32),
        name="project",
    )(wave_counts, moved, beta)


def couple(parts, weights):
    sources, rows, count = parts.shape
    shifts = weights.shape[0]
    bands = rows // 2
    most = (shifts + 1) // 2

    def kernel(parts_ref, weights_ref, low_ref, energy_ref):
        total = parts_ref[0]
        for s in range(1, sources):
            total = total + parts_ref[s]
        summed = jnp.zeros_like(total)
        for k in range(shifts):
            amount = (most - 1 - k) % count
            moved = total if amount == 0 else pltpu.roll(total, amount, 1)
            summed = summed + weights_ref[k : k + 1, :] * moved
        low_ref[...] = summed.astype(jnp.bfloat16)
        terms = total * summed
        energy = jnp.sum(terms[:bands] + terms[bands:], axis=1, keepdims=True)
        energy_ref[...] = jnp.broadcast_to(energy, energy_ref.shape)

    return pl.pallas_call(
        kernel,
        out_shape=(
            jax.ShapeDtypeStruct((rows, count), jnp.bfloat16),
            jax.ShapeDtypeStruct((bands, 128), jnp.float32),
        ),
        name="couple",
    )(parts, weights)


def apply(coupled, beta, wave_counts, tile):
    sources, rows, count = coupled.shape
    bands = rows // 2
    slots = beta.shape[2]

    def kernel(counts_ref, c_ref, beta_ref, out_ref):
        at = pl.program_id(0) * tile
        inside = lax.broadcasted_iota(jnp.int32, (bands, tile), 1) + at < counts_ref[0]
        left = c_ref[...].reshape(sources * rows, count)
        nn = (((1,), (0,)), ((), ()))
        first = lax.dot_general(left, beta_ref[0], nn, preferred_element_type=jnp.float32)
        second = lax.dot_general(left, beta_ref[1], nn, preferred_element_type=jnp.float32)
        for s in range(sources):
            re = slice(s * rows, s * rows + bands)
            im = slice(s * rows + bands, (s + 1) * rows)
            out_ref[s, 0] = jnp.where(inside, first[re] - second[im], 0.0).astype(jnp.bfloat16)
            out_ref[s, 1] = jnp.where(inside, first[im] + second[re], 0.0).astype(jnp.bfloat16)

    return pl.pallas_call(
        kernel,
        grid_spec=pltpu.PrefetchScalarGridSpec(
            num_scalar_prefetch=1,
            grid=(slots // tile,),
            in_specs=[
                pl.BlockSpec((sources, rows, count), lambda i, c: (0, 0, 0)),
                pl.BlockSpec((2, count, tile), lambda i, c: (0, 0, i)),
            ],
            out_specs=pl.BlockSpec((sources, 2, bands, tile), lambda i, c: (0, 0, 0, i)),
        ),
        out_shape=jax.ShapeDtypeStruct((sources, 2, bands, slots), jnp.bfloat16),
        name="apply",
    )(wave_counts, coupled, beta)


def shards(coeffs, projectors, block_coupling, atom_counts, wave_counts):
    own_bands = coeffs.shape[1]
    ga = lax.axis_size("ga")
    slots = projectors.shape[2]
    count = projectors.shape[0]
    sent = coeffs.reshape(2, own_bands, ga, slots).transpose(2, 0, 1, 3)
    moved = lax.all_to_all(sent, "ga", split_axis=0, concat_axis=0, tiled=True)
    beta = projectors.transpose(1, 0, 2)
    block_first, block_length = block_tables(atom_counts, lax.iota(jnp.int32, count))
    weights = shift_weights(block_first, block_length, block_coupling)
    partial = project(moved, beta, wave_counts, 256)
    parts = lax.all_to_all(partial, "ga", split_axis=0, concat_axis=0, tiled=True)
    low, energy = couple(parts, weights)
    band_energy = energy[:, 0] / count
    band_total = own_bands * ga * lax.axis_size("band")
    total_energy = lax.psum(jnp.sum(band_energy), ("ga", "band")) / math.sqrt(band_total)
    coupled = lax.all_gather(low, "ga", axis=0)
    result = apply(coupled, beta, wave_counts, 512)
    back = lax.all_to_all(result, "ga", split_axis=0, concat_axis=0, tiled=True)
    applied = back.transpose(1, 2, 0, 3).reshape(2, own_bands, ga * slots)
    return (applied, band_energy, total_energy)


def solution(mesh):
    placed = (P(None, ("ga", "band"), None), P(None, None, "ga"), P(), P(), P("ga"))
    return jax.shard_map(
        shards,
        mesh=mesh,
        in_specs=placed,
        out_specs=(P(None, ("ga", "band"), None), P(("ga", "band")), P()),
        check_vma=False,
    )
```
